32 devices in a mesh: row: 2 (over x), col: 4 (over z), depth: 4 (over y, core).
Axes of the slice: x: 2, y: 2, z: 4, core: 2. Of those that a mesh axis runs over, the one named last changes fastest.
Arguments:
- acts: bfloat16 [8192, 5120], P(('depth', 'col'), 'row'), may hold values from -6 to 6
- grad_out: bfloat16 [8192, 13824], P(('depth', 'row'), 'col'), may hold values from -6 to 6
- weight: bfloat16 [5120, 13824], P('row', 'col'), may hold values from -0.078125 to 0.078125
- master: float32 [5120, 13824], P(('row', 'depth'), 'col'), may hold values from -0.078125 to 0.078125
- moment_one: float32 [5120, 13824], P(('row', 'depth'), 'col'), may hold values from -4 to 4
- moment_two: float32 [5120, 13824], P(('row', 'depth'), 'col'), may hold values from 0.05 to 2
Outputs:
- grad_in: bfloat16 [8192, 5120], P(('depth', 'col'), 'row')
- new_weight: bfloat16 [5120, 13824], P('row', 'col')
- new_master: float32 [5120, 13824], P(('row', 'depth'), 'col')
- new_moment_one: float32 [5120, 13824], P(('row', 'depth'), 'col')
- new_moment_two: float32 [5120, 13824], P(('row', 'depth'), 'col')
The draws below stay inside these ranges and needn't reach their ends.
All inputs are finite; a program needn't handle non-finite values.
Results may differ from the reference program's by a relative error of at most 0.0035.
Values may be sent and summed in bfloat16 or wider, within the bound.
A program may use at most 192 MiB of HBM per device.

```python
import math
import jax
import jax.numpy as jnp
from jax import lax

D = 5120
FF = 13824
STEP = 10
TOKENS = 8192


def levels(own_key, dims, split, smallest, high):
    def one(position, blocks):
        draws = jax.random.uniform(jax.random.fold_in(jax.random.fold_in(own_key, 6), position), (blocks,), jnp.float32, smallest / len(split), high / len(split))
        return jnp.repeat(jnp.exp(draws), dims[position] // blocks).reshape((-1,) + (1,) * (len(dims) - position - 1))

    gain = one(*split[0])
    for cut in split[1:]:
        gain = gain * one(*cut)
    return gain


def gaussian(rng, shape, width, bound, pieces=(), held_as=jnp.bfloat16):
    drawn = jax.random.normal(rng, shape, jnp.float32) * width
    if len(pieces) > 0:
        drawn = levels(rng, shape, pieces, -0.22, 0.18) * drawn
    return jnp.clip(drawn, min=-bound, max=bound).astype(held_as)


def setup_inputs(seed: int = 0) -> dict:
    seeds = jax.random.split(jax.random.key(seed), 7)
    return {
        "acts": gaussian(seeds[0], (TOKENS, D), 1.0, 6.0, ((0, 16), (1, 2))),
        "grad_out": gaussian(seeds[1], (TOKENS, FF), 1.0, 6.0, ((0, 8), (1, 4))),
        "weight": gaussian(seeds[2], (D, FF), D ** -0.5, 0.078125, ((0, 2), (1, 4))),
        "master": gaussian(seeds[3], (D, FF), D ** -0.5, 0.078125, ((0, 8), (1, 4)), jnp.float32),
        "moment_one": gaussian(seeds[4], (D, FF), 0.3, 4.0, ((0, 8), (1, 4)), jnp.float32),
        "moment_two": jnp.clip(jnp.exp(math.log(2.0) - 3.6888794 * jax.random.uniform(seeds[5], (D, FF), jnp.float32) ** levels(seeds[5], (D, FF), ((0, 8), (1, 4)), -0.2, 0.2)), 0.05, 2.0),
    }


def reference(acts, grad_out, weight, master, moment_one, moment_two):
    grad_in = lax.dot_general(grad_out, weight, (((1,), (1,)), ((), ())), preferred_element_type=jnp.float32).astype(jnp.bfloat16)
    grad = lax.dot_general(acts, grad_out, (((0,), (0,)), ((), ())), preferred_element_type=jnp.float32)
    grad = grad * jnp.float32(1.0 / math.sqrt(TOKENS))
    new_moment_one = 0.9 * moment_one + 0.1 * grad
    new_moment_two = 0.95 * moment_two + 0.05 * grad * grad
    first_fix = 1.0 - 0.9 ** STEP
    second_fix = 1.0 - 0.95 ** STEP
    update = new_moment_one / first_fix / (jnp.sqrt(new_moment_two / second_fix) + 1e-08)
    new_master = master - 0.01 * (update + 0.1 * master)
    new_weight = new_master.astype(jnp.bfloat16)
    return (grad_in, new_weight, new_master, new_moment_one, new_moment_two)
```

```python
import functools
import math

import jax
import jax.numpy as jnp
from jax import lax
from jax.experimental import pallas as pl
from jax.sharding import PartitionSpec as P


STEP = 10
LANES = 128


def adamw(grad, master, moment_one, moment_two):
    new_moment_one = 0.9 * moment_one + 0.1 * grad
    new_moment_two = 0.95 * moment_two + 0.05 * grad * grad
    first_fix = 1.0 - 0.9**STEP
    second_fix = 1.0 - 0.95**STEP
    update = new_moment_one / first_fix / (jnp.sqrt(new_moment_two / second_fix) + 1e-08)
    new_master = master - 0.01 * (update + 0.1 * master)
    return new_master, new_moment_one, new_moment_two


def general(acts, grad_out, weight, master, moment_one, moment_two):
    whole_acts = lax.all_gather(acts, "col", axis=0, tiled=True)
    tokens_total = acts.shape[0] * lax.axis_size("col") * lax.axis_size("depth")
    whole_cotangent = lax.all_gather(grad_out, "row", axis=0, tiled=True)
    input_sum = lax.psum_scatter(
        lax.dot_general(
            whole_cotangent, weight, (((1,), (1,)), ((), ())), preferred_element_type=jnp.float32
        ),
        "col",
        scatter_dimension=0,
        tiled=True,
    )
    grad_sum = lax.psum_scatter(
        lax.dot_general(
            whole_acts, whole_cotangent, (((0,), (0,)), ((), ())), preferred_element_type=jnp.float32
        ).astype(jnp.bfloat16),
        "depth",
        scatter_dimension=0,
        tiled=True,
    ).astype(jnp.float32)
    grad = grad_sum * jnp.float32(1.0 / math.sqrt(tokens_total))
    updated = adamw(grad, master, moment_one, moment_two)
    new_weight = lax.all_gather(updated[0].astype(jnp.bfloat16), "depth", axis=0, tiled=True)
    return (input_sum.astype(jnp.bfloat16), new_weight) + updated


def update_kernel(scale, mine, near, far, master, one, two, *rest):
    out_master, out_one, out_two, out_weight = rest[-4:]
    f32 = jnp.float32
    grad = (mine[...].astype(f32) + near[...].astype(f32) + far[...].astype(f32)) * scale
    new_master, new_one, new_two = adamw(grad, master[...], one[...], two[...])
    out_master[...] = new_master
    out_one[...] = new_one
    out_two[...] = new_two
    out_weight[...] = new_master.astype(out_weight.dtype)


def update_chunk(scale, start, width, mine, near, far, state, previous):
    rows = mine.shape[0]
    block = LANES * math.gcd(start // LANES, width // LANES) if start else width
    while rows * block > 2**18 and block % (2 * LANES) == 0:
        block //= 2
    if rows * block > 2**18:
        block = LANES
    offset = start // block
    part = pl.BlockSpec((rows, block), lambda i: (0, i))
    placed = pl.BlockSpec((rows, block), lambda i: (0, i + offset))
    whole = jax.ShapeDtypeStruct(state[0].shape, state[0].dtype)
    return pl.pallas_call(
        functools.partial(update_kernel, scale),
        grid=(width // block,),
        in_specs=[part] * 3 + [placed] * 3 + [pl.BlockSpec(memory_space=pl.ANY)] * len(previous),
        out_specs=[placed] * 3 + [part],
        out_shape=[whole] * 3 + [jax.ShapeDtypeStruct((rows, width), jnp.bfloat16)],
        input_output_aliases={6 + i: i for i in range(len(previous))},
        cost_estimate=pl.CostEstimate(
            flops=20 * rows * width, bytes_accessed=32 * rows * width, transcendentals=rows * width
        ),
    )(mine, near, far, *state, *previous)


def cuts(columns, weights=(9, 9, 9)):
    units = columns // LANES
    total, at, result = sum(weights), 0, []
    run = 0
    for w in weights:
        run += w
        end = units * run // total
        result.append((at * LANES, (end - at) * LANES))
        at = end
    return result


def tie(value, *after):
    return lax.optimization_barrier((value,) + after)[0]


def per_device(*operands):
    return step(*operands)


def step(acts, grad_out, weight, master, moment_one, moment_two):
    f32, bf16 = jnp.float32, jnp.bfloat16
    cols, depths = lax.axis_size("col"), lax.axis_size("depth")
    row, col, depth = (lax.axis_index(a) for a in ("row", "col", "depth"))
    side, core = depth // 2, depth % 2
    tokens, width = acts.shape
    half, shard = width // 2, width // depths
    columns = grad_out.shape[1]
    scale = 1.0 / math.sqrt(tokens * cols * depths)
    swap_row = [(0, 1), (1, 0)]
    swap_side = [(0, 2), (2, 0), (1, 3), (3, 1)]
    swap_core = [(0, 1), (1, 0), (2, 3), (3, 2)]
    pieces = cuts(columns)

    far_cot = [
        lax.ppermute(lax.slice_in_dim(grad_out, s, s + w, axis=1), "row", swap_row)
        for s, w in pieces
    ]

    def input_rows(q):
        return lax.slice_in_dim(weight, q * half, (q + 1) * half, axis=0)

    def dot_in(cot, w):
        return lax.dot_general(cot, w, (((1,), (1,)), ((), ())), preferred_element_type=f32)

    heres = [dot_in(grad_out, input_rows(q)) for q in range(2)]

    def add_there(total, i, far):
        s, w = pieces[i]
        terms = [dot_in(far, lax.slice_in_dim(input_rows(q), s, s + w, axis=1)) for q in range(2)]
        return terms if total is None else [a + b for a, b in zip(total, terms)]

    there = add_there(None, 0, far_cot[0])

    def gather_line(block, after):
        rights, lefts = [block], [block]
        for s in range(1, cols):
            if s in after:
                rights[-1] = tie(rights[-1], *after[s])
                lefts[-1] = tie(lefts[-1], *after[s])
            rights.append(
                lax.ppermute(rights[-1], "col", [(i, i + 1) for i in range(s - 1, cols - 1)])
            )
            lefts.append(
                lax.ppermute(lefts[-1], "col", [(i, i - 1) for i in range(1, cols - s + 1)])
            )
        return rights, lefts

    def assemble(rights, lefts, *after):
        block = rights[0]
        rights = [tie(v, *after) for v in rights]
        lefts = [tie(v, *after) for v in lefts]
        out = jnp.zeros((cols * tokens, block.shape[1]), block.dtype)
        out = lax.dynamic_update_slice(out, block, (col * tokens, 0))
        for s in range(1, cols):
            picked = jnp.where(col >= s, rights[s], lefts[cols - s])
            at = lax.rem(col - s + cols, cols) * tokens
            out = lax.dynamic_update_slice(out, picked, (at, 0))
        return out

    def acts_of(which):
        return lax.dynamic_slice_in_dim(acts, which * half, half, axis=1)

    rights, lefts = gather_line(acts_of(1 - side), {2: (heres[0],), 3: (heres[1], *there)})
    acts_away = assemble(rights, lefts, heres[0])
    third_away = (rights[3], lefts[3])
    rights, lefts = gather_line(tie(acts_of(side), rights[2], lefts[2]), {})
    early_after = (rights[1], lefts[1])

    def grad_part(whole_acts, cot):
        out = lax.dot_general(
            whole_acts, cot, (((0,), (0,)), ((), ())), preferred_element_type=f32
        ).astype(bf16)
        mine = lax.dynamic_slice_in_dim(out, core * shard, shard, axis=0)
        give = lax.dynamic_slice_in_dim(out, (1 - core) * shard, shard, axis=0)
        return mine, lax.ppermute(give, "depth", swap_core)

    later_cot = tie(grad_out, heres[0])

    cots, sums = [], []
    for i, ((s, w), far) in enumerate(zip(pieces, far_cot)):
        if i == 0:
            far = tie(far, *there)
        if i == 1:
            far = tie(far, mine, *third_away)
        if i == 2:
            far = tie(far, mine, *there)
        near = lax.slice_in_dim(later_cot, s, s + w, axis=1)
        cot = jnp.zeros((2 * near.shape[0], w), near.dtype)
        cot = lax.dynamic_update_slice(cot, near, (row * near.shape[0], 0))
        cot = lax.dynamic_update_slice(cot, far, ((1 - row) * near.shape[0], 0))
        cots.append(cot)
        mine, near = grad_part(acts_away, cot)
        both = (mine.astype(f32) + near.astype(f32)).astype(bf16)
        sums.append(lax.ppermute(both, "depth", swap_side))
        if i > 0:
            there = add_there(there, i, tie(far, both))

    acts_home = assemble(rights, lefts, *there)

    state, previous = (master, moment_one, moment_two), ()
    new_weight = jnp.zeros(weight.shape, bf16)
    for (s, w), cot, far in zip(pieces, cots, sums):
        mine, near = grad_part(acts_home, cot)
        *previous, fresh = update_chunk(scale, s, w, mine, near, far, state, tuple(previous))
        across = lax.ppermute(fresh, "depth", swap_side)
        beside = lax.ppermute(fresh, "depth", swap_core)
        diagonal = lax.ppermute(across, "depth", swap_core)
        for block, a, b in (
            (fresh, side, core),
            (beside, side, 1 - core),
            (across, 1 - side, core),
            (diagonal, 1 - side, 1 - core),
        ):
            new_weight = lax.dynamic_update_slice(new_weight, block, ((2 * a + b) * shard, s))

    place = jnp.where(row == 0, col, cols - 1 - col)

    def hop(value, pairs):
        where = lambda r, m: r * cols + (m if r == 0 else cols - 1 - m)
        return lax.ppermute(
            value, ("row", "col"), [(where(r, a), where(r, b)) for r in (0, 1) for a, b in pairs]
        )

    def chain(first, second, at, flip):
        go = lambda v, pairs: hop(v, [(cols - 1 - a, cols - 1 - b) for a, b in pairs] if flip else pairs)
        got = go(first.astype(bf16), [(3, 2)])
        beside = go(second.astype(bf16), [(0, 1)])
        out = jnp.where(at == 3, second, first + got.astype(f32)).astype(bf16)
        got = go(out, [(3, 2), (2, 1)])
        out = (jnp.where(at == 1, first, second) + got.astype(f32)).astype(bf16)
        got = go(out, [(2, 1), (1, 0)])
        return beside.astype(f32) + got.astype(f32)

    def picked(block, first):
        return lax.dynamic_slice_in_dim(block, first * tokens, tokens, axis=0)

    outs = []
    for q in range(2):
        here = heres[q]
        p0, p1 = picked(here, row), picked(here, 1 - row)
        p2, p3 = picked(there[q], row), picked(there[q], 1 - row)
        q0, q1 = lax.optimization_barrier((p0, p1) + early_after)[:2]
        early = chain(q0, q1, place, False)
        late = chain(p3, p2, cols - 1 - place, True)
        own = jnp.where(place < 2, jnp.where(place == 0, p0, p1), jnp.where(place == 2, p2, p3))
        outs.append((own + jnp.where(place < 2, early, late)).astype(bf16))
    grad_in = jnp.concatenate(outs, axis=1)
    return (grad_in, new_weight) + tuple(previous)


def solution(mesh):
    shape = mesh.shape
    fits = shape["row"] == 2 and shape["col"] == 4 and shape["depth"] == 4
    state = P(("row", "depth"), "col")
    return jax.shard_map(
        per_device if fits else general,
        mesh=mesh,
        in_specs=(P(("depth", "col"), "row"), P(("depth", "row"), "col"), P("row", "col")) + (state,) * 3,
        out_specs=(P(("depth", "col"), "row"), P("row", "col")) + (state,) * 3,
        check_vma=False,
    )
```
